256 devices in a mesh: grp: 4 (over x, y), space: 64 (over z, core).
Axes of the slice: x: 2, y: 2, z: 32, core: 2. Of those that a mesh axis runs over, the one named last changes fastest.
The devices are a block of a 4x8x32 slice.
Arguments:
- propagator: bfloat16 [8, 3, 4, 12, 131072], P('grp', None, None, None, 'space'), parts along dimension 0, may hold values from -6 to 6
- eigvecs: bfloat16 [8, 3, 256, 131072], P('grp', None, None, 'space'), parts along dimension 0, may hold values from -16 to 16
- operator_weights: float32 [512, 2, 256], P('grp'), parts along dimension 0, may hold values from -0.375 to 0.375
- sink_time: int32 [4], P('grp'), parts along dimension 0, may hold values from 0 to 127
- term_index: int32 [48, 3], replicated, may hold values from 0 to 11
- term_sign: int32 [48], replicated, may hold values from 0 to 1
- solver_order: int32 [131072], P('space'), may hold values from 0 to 131071, as said below
Outputs:
- solver_source: bfloat16 [8, 3, 4, 12, 131072], P('grp', None, None, None, 'space'), parts along dimension 0
The draws below stay inside these ranges and needn't reach their ends.
There are 4 independent parts, one for each index of `grp`. The reference program is written for one: setup_inputs(seed, part) draws one part's arguments, and reference() takes and returns one part's arrays. A program takes and returns all parts, laid end to end along the dimension named above; an argument that names none is the same for every part. Nothing has to cross between parts.
Inputs may be any that keep to these rules, and one draw needn't show every extreme that they name: solver_order is a permutation of the sites; split into blocks of 2048 positions and each block into pieces of 32, piece d of block e holds only sites d * 2048 to (d + 1) * 2048 - 1.
All inputs are finite; a program needn't handle non-finite values.
Results may differ from the reference program's by a relative error of at most 0.006.
Values may be sent and summed in bfloat16 or wider, within the bound.
No kernel may reach another device: no remote copies, remote signals or barrier semaphores. Data moves between devices by JAX's collectives and lax.ppermute only.
A program may use at most 64 MiB of HBM per device.

```python
import math
import jax
import jax.numpy as jnp
from jax import lax

NVEC = 256
NMOM = 4
NTERM = 48
EXTENT = 64
TIME_EXTENT = 128
SITES_DEV = 2048
SITES = 131072
PAIR = 32


def one_permutation(block_key):
    return jax.random.permutation(block_key, SITES_DEV)


def draw_solver_order(key, part):
    owners_count = SITES // SITES_DEV
    block_keys = jax.random.split(jax.random.fold_in(key, 17), owners_count)
    shuffled = jax.vmap(one_permutation)(block_keys).astype(jnp.int32).reshape(owners_count, owners_count, PAIR)
    owner_start = (jnp.arange(owners_count, dtype=jnp.int32) * SITES_DEV)[:, None, None]
    ordered = (shuffled + owner_start).transpose(1, 0, 2)
    return ordered.reshape(SITES)


def place_ends(values, stream_key, smallest, top_value):
    spot = [jax.random.randint(jax.random.fold_in(stream_key, axis), (), 0, length) for axis, length in enumerate(values.shape)]
    main_axis = values.shape.index(max(values.shape))
    next_to = spot[:main_axis] + [(spot[main_axis] + 1) % values.shape[main_axis]] + spot[main_axis + 1:]
    return values.at[tuple(spot)].set(smallest).at[tuple(next_to)].set(top_value)


def spiked(entries, own_key, source, target, blocks, factor):
    def block_of(dim):
        return (jnp.arange(entries.shape[dim]) // (entries.shape[dim] // blocks)).reshape((-1,) + (1,) * (entries.ndim - 1 - dim))

    near = jax.random.permutation(own_key, blocks)[block_of(target)]
    far = (block_of(target) + blocks // 2) % blocks
    return jnp.where((block_of(source) == near) | (block_of(source) == far), factor * entries, entries)


def steps_of(rng, extent, shards, smallest, top_value):
    loudness = 1.0
    for position, parts in shards:
        draws = jax.random.uniform(jax.random.fold_in(jax.random.fold_in(rng, 6), position), (parts,), jnp.float32, smallest / len(shards), top_value / len(shards))
        loudness = loudness * jnp.repeat(jnp.exp(draws), extent[position] // parts).reshape((-1,) + (1,) * (len(extent) - 1 - position))
    return loudness


def normal_values(own_key, dims, scale, bound, cuts=(), kind=jnp.bfloat16):
    result = jax.random.normal(own_key, dims, jnp.float32) * scale
    if len(cuts) > 0:
        result = steps_of(own_key, dims, cuts, -0.22, 0.18) * result
    return jnp.clip(result, min=-bound, max=bound).astype(kind)


def gaussian_with(key, dims, spread, limit, cuts, heavy, held_as=jnp.bfloat16):
    values = spread * jax.random.normal(key, dims, jnp.float32)
    if cuts:
        values = values * steps_of(key, dims, cuts, -0.22, 0.18)
    return jnp.clip(spiked(values, jax.random.fold_in(key, 3), *heavy), -limit, limit).astype(held_as)


def setup_inputs(seed: int = 0, part: int = 0) -> dict:
    splits = jax.random.split(jax.random.key(seed), 8)
    part_splits = jax.random.split(jax.random.fold_in(splits[7], part), 8)
    return {
        "propagator": normal_values(part_splits[0], (2, 3, 4, 12, SITES), 1.0, 6.0, ((4, 64),)),
        "eigvecs": gaussian_with(part_splits[1], (2, 3, NVEC, SITES), 1.0, 16.0, ((3, 64),), (3, 2, 64, 4.0)),
        "operator_weights": normal_values(part_splits[2], (TIME_EXTENT, 2, NVEC), NVEC ** -0.5, 0.375, (), jnp.float32),
        "sink_time": jax.random.randint(part_splits[3], (1,), 0, TIME_EXTENT).astype(jnp.int32),
        "term_index": place_ends(jax.random.randint(splits[4], (NTERM, 3), 0, 12), jax.random.fold_in(splits[4], 1), 0, 11).astype(jnp.int32),
        "term_sign": place_ends(jax.random.randint(splits[5], (NTERM,), 0, 2), jax.random.fold_in(splits[5], 1), 0, 1).astype(jnp.int32),
        "solver_order": draw_solver_order(jax.random.fold_in(splits[7], 71), part),
    }


MOMENTA = ((0, 0, 0), (1, 0, 0), (0, 1, 0), (0, 0, 1))
PRECISE = lax.Precision.HIGHEST

def phase_tables(offset, length):
    site_index = offset + jnp.arange(length, dtype=jnp.int32)
    coord_x = site_index % EXTENT
    coord_y = site_index // EXTENT % EXTENT
    coord_z = site_index // (EXTENT * EXTENT)
    windings = jnp.stack([(step_x * coord_x + step_y * coord_y + step_z * coord_z) % EXTENT for step_x, step_y, step_z in MOMENTA])
    angles = windings.astype(jnp.float32) * (2.0 * math.pi / EXTENT)
    return (jnp.cos(angles), jnp.sin(angles))

def phased_rows(prop_colour, cosine_table, sine_table):
    real_part = prop_colour[0].astype(jnp.float32)[None]
    imag_part = prop_colour[1].astype(jnp.float32)[None]
    cos_rows = cosine_table[:, None, None, :]
    sin_rows = sine_table[:, None, None, :]
    turned = jnp.stack([cos_rows * real_part + sin_rows * imag_part, cos_rows * imag_part - sin_rows * real_part])
    return turned.astype(jnp.bfloat16).reshape(-1, turned.shape[-1])

def project(eig_colour, phased, scale_in):
    from_real = jnp.dot(eig_colour[0], phased.T, preferred_element_type=jnp.float32).reshape(-1, 2, NMOM, 48)
    from_imag = jnp.dot(eig_colour[1], phased.T, preferred_element_type=jnp.float32).reshape(-1, 2, NMOM, 48)
    real_part = from_real[:, 0] + from_imag[:, 1]
    imag_part = from_real[:, 1] - from_imag[:, 0]
    return jnp.stack([real_part, imag_part]) * scale_in

def assemble(pieces):
    stacked = jnp.stack(pieces)
    vectors = stacked.shape[2]
    return stacked.transpose(3, 1, 2, 0, 4).reshape(NMOM, 2, vectors, 144)

def weighted_total(blocks, weights):
    real_sum = jnp.einsum('k,pkc->pc', weights[0], blocks[:, 0], precision=PRECISE) - jnp.einsum('k,pkc->pc', weights[1], blocks[:, 1], precision=PRECISE)
    imag_sum = jnp.einsum('k,pkc->pc', weights[0], blocks[:, 1], precision=PRECISE) + jnp.einsum('k,pkc->pc', weights[1], blocks[:, 0], precision=PRECISE)
    return jnp.stack([real_sum, imag_sum], axis=1)

def term_tables(term_index, term_sign):
    channels = jnp.arange(12, dtype=jnp.int32)
    first_pick = (term_index[:, 0:1] == channels[None]).astype(jnp.float32)
    second_pick = (term_index[:, 1:2] == channels[None]).astype(jnp.float32)
    sign_values = (2 * term_sign - 1).astype(jnp.float32)
    placement = (term_index[None, :, 2] == channels[:, None]).astype(jnp.float32) * sign_values[None]
    return (first_pick, second_pick, placement)

def contract(blocks, weighted, first_pick, second_pick, placement):
    vectors = blocks.shape[2]
    block_grid = blocks.reshape(NMOM, 2, vectors, 12, 12)
    first_terms = jnp.einsum('mi,pqkij->pqkmj', first_pick, block_grid, precision=PRECISE)
    second_terms = jnp.einsum('mi,pqij->pqmj', second_pick, weighted.reshape(NMOM, 2, 12, 12), precision=PRECISE)[:, :, None]
    real_part = first_terms[:, 0] * second_terms[:, 0] - first_terms[:, 1] * second_terms[:, 1]
    imag_part = first_terms[:, 0] * second_terms[:, 1] + first_terms[:, 1] * second_terms[:, 0]
    product = jnp.stack([real_part, imag_part], axis=1)
    return jnp.einsum('cm,pqkmj->pqkcj', placement, product, precision=PRECISE).reshape(NMOM, 2, vectors, 144)

def rebuild(coeffs, eig_colour, colour, cosine_table, sine_table, scale_out):
    vectors = coeffs.shape[2]
    colour_block = coeffs.reshape(NMOM, 2, vectors, 3, 48)[:, :, :, colour]
    coeff_table = colour_block.transpose(2, 1, 0, 3).reshape(vectors, 2 * NMOM * 48)
    from_real = jnp.dot(coeff_table.T, eig_colour[0], preferred_element_type=jnp.float32).reshape(2, NMOM, 48, -1)
    from_imag = jnp.dot(coeff_table.T, eig_colour[1], preferred_element_type=jnp.float32).reshape(2, NMOM, 48, -1)
    real_part = from_real[0] - from_imag[1]
    imag_part = from_real[1] + from_imag[0]
    cos_rows = cosine_table[:, None, :]
    sin_rows = sine_table[:, None, :]
    out_real = lax.optimization_barrier(jnp.sum(cos_rows * real_part - sin_rows * imag_part, axis=0))
    out_imag = lax.optimization_barrier(jnp.sum(cos_rows * imag_part + sin_rows * real_part, axis=0))
    return jnp.stack([out_real, out_imag]) * scale_out

def reference(propagator, eigvecs, operator_weights, sink_time, term_index, term_sign, solver_order):
    cosine_table, sine_table = phase_tables(0, SITES)
    scale_in = 1.0 / math.sqrt(3.0 * SITES)
    pieces = []
    for colour in range(3):
        phased = phased_rows(propagator[:, colour], cosine_table, sine_table)
        pieces.append(project(eigvecs[:, colour], phased, scale_in))
    blocks = assemble(pieces)
    weights = lax.dynamic_index_in_dim(operator_weights, sink_time[0], 0, keepdims=False)
    first_pick, second_pick, placement = term_tables(term_index, term_sign)
    weighted = weighted_total(blocks, weights)
    coeffs = contract(blocks, weighted, first_pick, second_pick, placement).astype(jnp.bfloat16)
    scale_out = 1.0 / math.sqrt(NMOM * NVEC)
    colours = [rebuild(coeffs, eigvecs[:, colour], colour, cosine_table, sine_table, scale_out) for colour in range(3)]
    source = jnp.stack(colours, axis=1).astype(jnp.bfloat16).reshape(2, 3, 4, 12, SITES)
    return jnp.take(source, solver_order, axis=4)
```

```python
import functools
import math

import jax
import jax.numpy as jnp
from jax import lax
from jax.experimental import pallas as pl
from jax.experimental.pallas import tpu as pltpu
from jax.sharding import Mesh
from jax.sharding import PartitionSpec as P

NMOM = 4
NTERM = 48
EXTENT = 64
NEAR = 8
NEAR_OFFSETS = (4, 3, -3, 2, -2, 1, -1)
SOURCES = (0, *NEAR_OFFSETS)
DIGIT = 64


F32 = jnp.float32
BF16 = jnp.bfloat16


def lanes_of(shape):
    return lax.broadcasted_iota(jnp.int32, shape, len(shape) - 1)


def half_swap(x):
    return pltpu.roll(x, 64, x.ndim - 1)


def other_part(tiles):
    first, second, third = tiles
    low = lanes_of(first.shape) < 64
    return [
        half_swap(jnp.where(low, third, second)),
        half_swap(jnp.where(low, first, third)),
        half_swap(jnp.where(low, second, first)),
    ]


def with_signs(tiles):
    first, second, third = tiles
    return [-first, jnp.where(lanes_of(second.shape) < 64, -second, second), third]


def pick(which, options):
    out = options[0]
    for n, option in enumerate(options[1:], 1):
        out = jnp.where(which == n, option, out)
    return out


def project_kernel(meta, prop, eig, weights, send, keep, weighted, table, phased, halves, rows):
    colour = pl.program_id(0)
    length = prop.shape[-1]
    core = meta[2]

    @pl.when(colour == 0)
    def _():
        site = (2 * meta[1] + core) * length + lanes_of((8, length))
        row = lax.broadcasted_iota(jnp.int32, (8, length), 0)
        momentum = row % NMOM
        coord_x = site % EXTENT
        coord_y = site // EXTENT % EXTENT
        coord_z = site // (EXTENT * EXTENT) % EXTENT
        winding = jnp.where(
            momentum == 1,
            coord_x,
            jnp.where(momentum == 2, coord_y, jnp.where(momentum == 3, coord_z, 0)),
        )
        angle = winding.astype(F32) * (2.0 * math.pi / EXTENT)
        table[...] = jnp.where(row < NMOM, jnp.cos(angle), jnp.sin(angle))

    for part in range(2):
        for j in range(12):
            rows[part, 4 * j : 4 * j + 4, :] = prop[part, 0, j].astype(F32)
    real = rows[0]
    imag = rows[1]
    for p in range(NMOM):
        if p == 0:
            turned = (real, imag)
        else:
            cosine = table[p : p + 1, :]
            sine = table[NMOM + p : NMOM + p + 1, :]
            turned = (cosine * real + sine * imag, cosine * imag - sine * real)
        phased[48 * p : 48 * p + 48, :] = turned[0].astype(BF16)
        phased[192 + 48 * p : 240 + 48 * p, :] = turned[1].astype(BF16)
    both = eig[:, 0].reshape(-1, length)
    vectors = both.shape[0] // 2
    product = lax.dot_general(
        both, phased[...], (((1,), (1,)), ((), ())), preferred_element_type=F32
    )
    from_real = [product[:vectors, 128 * n : 128 * n + 128] for n in range(3)]
    from_imag = [product[vectors:, 128 * n : 128 * n + 128] for n in range(3)]
    turned = with_signs(other_part(from_imag))
    tiles = [x - y for x, y in zip(from_real, turned)]
    sums = lax.dot_general(
        weights[0],
        jnp.concatenate(tiles, axis=1),
        (((1,), (0,)), ((), ())),
        precision=lax.Precision.HIGHEST,
        preferred_element_type=F32,
    )
    by_real = [sums[0:1, 128 * n : 128 * n + 128] for n in range(3)]
    by_imag = [sums[1:2, 128 * n : 128 * n + 128] for n in range(3)]
    weighted[0] = jnp.zeros((8, 128), F32)
    for n, turned in enumerate(with_signs(other_part(by_imag))):
        weighted[0, n : n + 1, :] = by_real[n] + turned
    for n, tile in enumerate(tiles):
        halves[...] = tile.reshape(halves.shape)
        keep[n] = halves[core]
        send[n] = halves[1 - core]


def in_two(x):
    high = x.astype(BF16).astype(F32)
    return high, x - high


def split_kernel(meta, keep, other, own_sum, other_sum, wanted, *outs):
    sums = [own_sum[a, 0:3, :] + other_sum[a, 0:3, :] for a in range(3)]
    high, low = in_two(jnp.concatenate([*sums, jnp.zeros((7, 128), F32)], axis=0))
    for offset, out in zip(SOURCES, outs):
        slot = (meta[1] + offset + NEAR) % NEAR
        tail = jnp.concatenate(
            [high[0:9], low[0:9], wanted[slot].astype(F32), jnp.zeros((2, 128), F32)], axis=0
        )
        for n in range(9):
            out[n] = (keep[n, slot] + other[n, slot]).astype(out.dtype)
        out[9] = tail[0:16].astype(out.dtype)
        out[10] = jnp.concatenate([tail[16:24], jnp.zeros((8, 128), F32)], axis=0).astype(out.dtype)


def near_kernel(meta, *refs):
    given, outs = (refs[:8], refs[8:12])
    far = meta[1] // NEAR
    tails = [
        jnp.concatenate([g[9].astype(F32), g[10, 0:8].astype(F32)], axis=0) for g in given
    ]
    high, low = in_two(sum(t[0:9] + t[9:18] for t in tails))
    for n in range(9):
        total = sum(g[n].astype(F32) for g in given)
        for out in outs:
            out[n] = total.astype(out.dtype)
    for step, out in enumerate(outs):
        dest = (far + step) % 4
        asked = [pick(dest, [t[18 + m : 19 + m] for m in range(4)]) for t in tails]
        rows = jnp.concatenate([high, low, *asked, jnp.zeros((6, 128), F32)], axis=0)
        out[9] = rows[0:16].astype(out.dtype)
        out[10] = rows[16:32].astype(out.dtype)


def contract_kernel(meta, index, sign, *refs, scale, places):
    given, coeffs, wanted, plain, swapped, w_real, w_imag, total = (refs[:4], *refs[4:11])
    sums = jnp.zeros((9, 128), F32)
    for step, g in enumerate(given):
        tail = jnp.concatenate([g[9].astype(F32), g[10].astype(F32)], axis=0)
        sums = sums + (tail[0:9] + tail[9:18])
        for n, offset in enumerate(SOURCES):
            source = (meta[1] - NEAR * step - offset + 2 * places) % places
            wanted[source] = tail[18 + n : 19 + n]
    sums = sums * scale
    for a in range(3):
        tiles = [sum(g[3 * a + n].astype(F32) for g in given) * scale for n in range(3)]
        rows = [jnp.broadcast_to(sums[3 * a + n : 3 * a + n + 1], (16, 128)) for n in range(3)]
        turned = other_part(tiles)
        w_turned = other_part(rows)
        low = lanes_of((16, 128)) < 64
        real = [rows[0], jnp.where(low, rows[1], w_turned[1]), w_turned[2]]
        imag = [-w_turned[0], jnp.where(low, -w_turned[1], rows[1]), rows[2]]
        for alpha in range(4):
            i = 4 * a + alpha
            for n in range(3):
                for to, x in ((plain, tiles), (swapped, turned), (w_real, real), (w_imag, imag)):
                    to[i, n] = x[n] if alpha == 0 else pltpu.roll(x[n], 128 - alpha, 1)
    total[...] = jnp.zeros(total.shape, F32)

    def term(m, carry):
        first, second, out = (index[3 * m], index[3 * m + 1], index[3 * m + 2])
        signed = (2 * sign[m] - 1).astype(F32)
        value = plain[first] * w_real[second] + swapped[first] * w_imag[second]
        total[out] = total[out] + signed * value
        return carry

    lax.fori_loop(0, NTERM, term, 0, unroll=4)
    place = lanes_of((16, 128)) % 4
    for a in range(3):
        for n in range(3):
            moved = [total[4 * a, n]] + [
                pltpu.roll(total[4 * a + alpha, n], alpha, 1) for alpha in range(1, 4)
            ]
            coeffs[3 * a + n] = pick(place, moved).astype(BF16)


def rebuild_kernel(meta, *refs, scale):
    ours, theirs = (refs[:8], refs[8:16])
    eig, table, wanted, out, coeffs, source = refs[16:]
    step = pl.program_id(0)
    length = eig.shape[-1]

    @pl.when(step == 0)
    def _():
        for side, group in ((meta[2], ours), (1 - meta[2], theirs)):
            for offset, g in zip(SOURCES, group):
                slot = (meta[1] - offset + NEAR) % NEAR
                for n in range(9):
                    coeffs[n, side, slot] = g[n]

    @pl.when(step < 3)
    def _():
        vectors = eig.shape[2]
        dense = [coeffs[3 * step + n].reshape(vectors, 128).astype(F32) for n in range(3)]
        both = eig[:, 0].reshape(-1, length)
        turned = with_signs(other_part(dense))
        left = jnp.concatenate(
            [jnp.concatenate([x.T, y.T], axis=1) for x, y in zip(dense, turned)], axis=0
        ).astype(BF16)
        product = jnp.dot(left, both, preferred_element_type=F32)
        real = product[0:48]
        imag = product[192:240]
        for p in range(1, NMOM):
            cosine = table[p : p + 1, :]
            sine = table[NMOM + p : NMOM + p + 1, :]
            part_real = product[48 * p : 48 * p + 48]
            part_imag = product[192 + 48 * p : 240 + 48 * p]
            real = real + (cosine * part_real - sine * part_imag)
            imag = imag + (cosine * part_imag + sine * part_real)
        source[0, step] = (real * scale).astype(BF16)
        source[1, step] = (imag * scale).astype(BF16)

    @pl.when(step >= 3)
    def _():
        group = step - 3
        low_half = lanes_of((1, 128)) < 64
        segment = lanes_of((72, 128)) // 32
        sites = lax.broadcasted_iota(jnp.int32, (length, 128), 0)
        hots = []
        for t in range(2):
            row_a = wanted[4 * group + 2 * t]
            row_b = wanted[4 * group + 2 * t + 1]
            local_a = row_a * DIGIT + half_swap(row_a)
            local_b = half_swap(row_b) * DIGIT + row_b
            local = jnp.where(low_half, local_a, local_b).astype(jnp.int32)
            hots.append(jnp.where(sites == local, 1.0, 0.0).astype(BF16))
        hot = jnp.concatenate(hots, axis=1)
        picked = jnp.dot(source[...].reshape(-1, length), hot, preferred_element_type=F32)
        for t in range(2):
            blocks = [
                picked[72 * q : 72 * q + 72, 128 * t : 128 * t + 128] for q in range(4)
            ]
            for s in range(4):
                out[4 * t + s] = pick(
                    segment,
                    [
                        blocks[q] if q == s else pltpu.roll(blocks[q], 32 * (q - s) % 128, 1)
                        for q in range(4)
                    ],
                ).astype(BF16)


def place_kernel(given, out):
    segment = lanes_of((72, 128)) // 32
    for t in range(out.shape[-1] // 128):
        blocks = [given[4 * t + s].astype(F32) for s in range(4)]
        for q in range(4):
            mixed = pick(
                segment,
                [
                    blocks[s] if q == s else pltpu.roll(blocks[s], 32 * (s - q) % 128, 1)
                    for s in range(4)
                ],
            ).astype(BF16)
            for n in range(18):
                part, colour, j = ((18 * q + n) // 36, (18 * q + n) // 12 % 3, (18 * q + n) % 12)
                out[part, colour, j, :, 128 * t : 128 * t + 128] = mixed[4 * n : 4 * n + 4]


def shape_of(shape, dtype):
    return jax.ShapeDtypeStruct(shape, dtype)


def whole(count):
    return [pl.BlockSpec(memory_space=pltpu.VMEM)] * count


def small_call(kernel, scalars, arrays, outs, scratch=(), name=None):
    out_shape = [shape_of(*o) for o in outs]
    return pl.pallas_call(
        kernel,
        grid_spec=pltpu.PrefetchScalarGridSpec(
            num_scalar_prefetch=len(scalars),
            grid=(),
            in_specs=whole(len(arrays)),
            out_specs=whole(len(outs)),
            scratch_shapes=list(scratch),
        ),
        out_shape=out_shape,
        name=name,
    )(*scalars, *arrays)


def on_device(
    propagator, eigvecs, operator_weights, sink_time, term_index, term_sign, solver_order
):
    length = propagator.shape[-1]
    vectors = eigvecs.shape[2]
    places = lax.axis_size("z")
    devices = 2 * places
    z = lax.axis_index("z")
    core = lax.axis_index("core")
    meta = jnp.stack([sink_time[0], z, core]).astype(jnp.int32)
    scale_in = 1.0 / math.sqrt(3.0 * length * devices)
    scale_out = 1.0 / math.sqrt(NMOM * vectors)

    def shifted(x, offset):
        return lax.ppermute(x, "z", [(n, (n + offset) % places) for n in range(places)])

    def swapped(x):
        return lax.ppermute(x, "core", [(0, 1), (1, 0)])

    half = (vectors // 2 // 16, 16, 128)
    send, keep, weighted, table = pl.pallas_call(
        project_kernel,
        grid_spec=pltpu.PrefetchScalarGridSpec(
            num_scalar_prefetch=1,
            grid=(3,),
            in_specs=[
                pl.BlockSpec((2, 1, 12, 4, length), lambda a, m: (0, a, 0, 0, 0)),
                pl.BlockSpec((2, 1, vectors, length), lambda a, m: (0, a, 0, 0)),
                pl.BlockSpec((1, 2, vectors), lambda a, m: (m[0], 0, 0)),
            ],
            out_specs=[
                pl.BlockSpec((3, *half), lambda a, m: (a, 0, 0, 0)),
                pl.BlockSpec((3, *half), lambda a, m: (a, 0, 0, 0)),
                pl.BlockSpec((1, 8, 128), lambda a, m: (a, 0, 0)),
                pl.BlockSpec((8, length), lambda a, m: (0, 0)),
            ],
            scratch_shapes=[
                pltpu.VMEM((384, length), BF16),
                pltpu.VMEM((2, *half), F32),
                pltpu.VMEM((2, 48, length), F32),
            ],
        ),
        out_shape=[
            shape_of((9, *half), F32),
            shape_of((9, *half), F32),
            shape_of((3, 8, 128), F32),
            shape_of((8, length), F32),
        ],
        name="project",
    )(meta, propagator.transpose(0, 1, 3, 2, 4), eigvecs, operator_weights)

    local = solver_order.reshape(4, NEAR, 2, 1, devices // 2) % length
    digits = jnp.concatenate([local // DIGIT, local % DIGIT], axis=3).astype(BF16)
    by_core = digits.transpose(2, 1, 0, 3, 4)
    mine = lax.dynamic_index_in_dim(by_core, core, 0, keepdims=False)
    partners = swapped(lax.dynamic_index_in_dim(by_core, 1 - core, 0, keepdims=False))
    first = jnp.where(core == 0, mine, partners)
    second = jnp.where(core == 0, partners, mine)
    wanted = jnp.stack([first, second], axis=3).reshape(NEAR, 4, 128)

    message = (11, 16, 128)
    split = small_call(
        split_kernel,
        [meta],
        [keep, swapped(send), weighted, swapped(weighted), wanted],
        [(message, F32)] + [(message, BF16)] * 7,
        name="split",
    )
    near = [split[0]] + [shifted(x, o) for x, o in zip(split[1:], NEAR_OFFSETS)]
    steps = (0, 2, 1, 3)
    far = small_call(near_kernel, [meta], near, [(message, F32)] + [(message, BF16)] * 3, name="near")
    arrived = {0: far[0]} | {n: shifted(far[n], NEAR * n - places * (n == 3)) for n in (2, 1, 3)}
    wide = pltpu.VMEM((12, 3, 16, 128), F32)
    coeffs, places_wanted = small_call(
        functools.partial(contract_kernel, scale=scale_in, places=places),
        [meta, term_index.reshape(-1), term_sign],
        [arrived[n] for n in range(4)],
        [((9, 16, 128), BF16), ((places, 1, 128), F32)],
        [wide] * 5,
        name="contract",
    )
    ours = [coeffs] + [shifted(coeffs, o) for o in NEAR_OFFSETS]
    theirs = [swapped(x) for x in ours]

    packed = pl.pallas_call(
        functools.partial(rebuild_kernel, scale=scale_out),
        grid_spec=pltpu.PrefetchScalarGridSpec(
            num_scalar_prefetch=1,
            grid=(3 + devices // 8,),
            in_specs=whole(16)
            + [
                pl.BlockSpec(
                    (2, 1, vectors, length), lambda s, m: (0, jnp.minimum(s, 2), 0, 0)
                ),
                pl.BlockSpec(memory_space=pltpu.VMEM),
                pl.BlockSpec(memory_space=pltpu.VMEM),
            ],
            out_specs=pl.BlockSpec(
                (8, 72, 128), lambda s, m: (jnp.maximum(s - 3, 0), 0, 0)
            ),
            scratch_shapes=[
                pltpu.VMEM((9, 2, *half), BF16),
                pltpu.VMEM((2, 3, 48, length), BF16),
            ],
        ),
        out_shape=shape_of((devices, 72, 128), BF16),
        name="rebuild",
    )(meta, *ours, *theirs, eigvecs, table, places_wanted)
    moved = lax.all_to_all(packed, ("z", "core"), 0, 0, tiled=True)
    tiles = 4
    placed = pl.pallas_call(
        place_kernel,
        grid=(length // (128 * tiles),),
        in_specs=[pl.BlockSpec((4 * tiles, 72, 128), lambda t: (t, 0, 0))],
        out_specs=pl.BlockSpec((2, 3, 12, 4, 128 * tiles), lambda t: (0, 0, 0, 0, t)),
        out_shape=shape_of((2, 3, 12, 4, length), BF16),
        name="place",
    )(moved)
    return placed.transpose(0, 1, 3, 2, 4)


def solution(mesh):
    shape = (mesh.shape["grp"], mesh.shape["space"] // 2, 2)
    finer = Mesh(mesh.devices.reshape(shape), ("grp", "z", "core"))
    space = ("z", "core")
    in_specs = (
        P("grp", None, None, None, space),
        P("grp", None, None, space),
        P("grp", None, None),
        P("grp"),
        P(),
        P(),
        P(space),
    )
    out_specs = P("grp", None, None, None, space)
    return jax.shard_map(
        on_device, mesh=finer, in_specs=in_specs, out_specs=out_specs, check_vma=False
    )
```

```python
import functools
import math

import jax
import jax.numpy as jnp
from jax import lax
from jax.experimental import pallas as pl
from jax.experimental.pallas import tpu as pltpu
from jax.sharding import Mesh
from jax.sharding import PartitionSpec as P


NMOM = 4
NTERM = 48
EXTENT = 64
NEAR = 8
NEAR_OFFSETS = (4, 3, -3, 2, -2, 1, -1)
SOURCES = (0, *NEAR_OFFSETS)
DIGIT = 64
HOPS = tuple(side * r for r in range(NEAR - 1, 0, -1) for side in (1, -1))


F32 = jnp.float32
BF16 = jnp.bfloat16


def lanes_of(shape):
    return lax.broadcasted_iota(jnp.int32, shape, len(shape) - 1)


def half_swap(x):
    return pltpu.roll(x, 64, x.ndim - 1)


def other_part(tiles):
    first, second, third = tiles
    low = lanes_of(first.shape) < 64
    return [
        half_swap(jnp.where(low, third, second)),
        half_swap(jnp.where(low, first, third)),
        half_swap(jnp.where(low, second, first)),
    ]


def with_signs(tiles):
    first, second, third = tiles
    return [-first, jnp.where(lanes_of(second.shape) < 64, -second, second), third]


def pick(which, options):
    out = options[0]
    for n, option in enumerate(options[1:], 1):
        out = jnp.where(which == n, option, out)
    return out


def project_kernel(meta, prop, eig, weights, asked, send, keep, weighted, table, phased, halves, rows):
    colour = pl.program_id(0)
    length = prop.shape[-1]
    core = meta[2]

    @pl.when(colour == 0)
    def _():
        site = (2 * meta[1] + core) * length + lanes_of((8, length))
        row = lax.broadcasted_iota(jnp.int32, (8, length), 0)
        momentum = row % NMOM
        coord_x = site % EXTENT
        coord_y = site // EXTENT % EXTENT
        coord_z = site // (EXTENT * EXTENT) % EXTENT
        winding = jnp.where(
            momentum == 1,
            coord_x,
            jnp.where(momentum == 2, coord_y, jnp.where(momentum == 3, coord_z, 0)),
        )
        angle = winding.astype(F32) * (2.0 * math.pi / EXTENT)
        table[...] = jnp.where(row < NMOM, jnp.cos(angle), jnp.sin(angle))
        send[9] = jnp.zeros(send.shape[1:], F32)
        for slot in range(NEAR):
            send[9, slot, 8:12, :] = asked[slot]

    for part in range(2):
        for j in range(12):
            rows[part, 4 * j : 4 * j + 4, :] = prop[part, 0, j].astype(F32)
    real = rows[0]
    imag = rows[1]
    for p in range(NMOM):
        if p == 0:
            turned = (real, imag)
        else:
            cosine = table[p : p + 1, :]
            sine = table[NMOM + p : NMOM + p + 1, :]
            turned = (cosine * real + sine * imag, cosine * imag - sine * real)
        phased[48 * p : 48 * p + 48, :] = turned[0].astype(BF16)
        phased[192 + 48 * p : 240 + 48 * p, :] = turned[1].astype(BF16)
    both = eig[:, 0].reshape(-1, length)
    vectors = both.shape[0] // 2
    product = lax.dot_general(
        both, phased[...], (((1,), (1,)), ((), ())), preferred_element_type=F32
    )
    from_real = [product[:vectors, 128 * n : 128 * n + 128] for n in range(3)]
    from_imag = [product[vectors:, 128 * n : 128 * n + 128] for n in range(3)]
    turned = with_signs(other_part(from_imag))
    tiles = [x - y for x, y in zip(from_real, turned)]
    sums = lax.dot_general(
        weights[0],
        jnp.concatenate(tiles, axis=1),
        (((1,), (0,)), ((), ())),
        precision=lax.Precision.HIGHEST,
        preferred_element_type=F32,
    )
    by_real = [sums[0:1, 128 * n : 128 * n + 128] for n in range(3)]
    by_imag = [sums[1:2, 128 * n : 128 * n + 128] for n in range(3)]
    weighted[0] = jnp.zeros((8, 128), F32)
    for n, turned in enumerate(with_signs(other_part(by_imag))):
        weighted[0, n : n + 1, :] = by_real[n] + turned
    send[9, colour, 0:8, :] = weighted[0]
    for n, tile in enumerate(tiles):
        halves[...] = tile.reshape(halves.shape)
        keep[n] = halves[core]
        send[3 * colour + n] = halves[1 - core]


def in_two(x):
    high = x.astype(BF16).astype(F32)
    return high, x - high


def split_kernel(meta, keep, other, own_sum, asked, *outs):
    sums = [own_sum[a, 0:3, :] + other[9, a, 0:3, :] for a in range(3)]
    high, low = in_two(jnp.concatenate([*sums, jnp.zeros((7, 128), F32)], axis=0))
    for offset, out in zip(SOURCES, outs):
        slot = (meta[1] + offset + NEAR) % NEAR
        pair = (asked[slot], other[9, slot, 8:12, :])
        wanted = pick(meta[2], pair) + pltpu.roll(pick(meta[2], pair[::-1]), 32, 1)
        tail = jnp.concatenate(
            [high[0:9], low[0:9], wanted, jnp.zeros((2, 128), F32)], axis=0
        )
        for n in range(9):
            out[n] = (keep[n, slot] + other[n, slot]).astype(out.dtype)
        out[9] = tail[0:16].astype(out.dtype)
        out[10] = jnp.concatenate([tail[16:24], jnp.zeros((8, 128), F32)], axis=0).astype(out.dtype)


def near_kernel(meta, *refs):
    given, outs = (refs[:8], refs[8:12])
    far = meta[1] // NEAR
    tails = [
        jnp.concatenate([g[9].astype(F32), g[10, 0:8].astype(F32)], axis=0) for g in given
    ]
    high, low = in_two(sum(t[0:9] + t[9:18] for t in tails))
    for n in range(9):
        total = sum(g[n].astype(F32) for g in given)
        for out in outs:
            out[n] = total.astype(out.dtype)
    for step, out in enumerate(outs):
        dest = (far + step) % 4
        asked = [pick(dest, [t[18 + m : 19 + m] for m in range(4)]) for t in tails]
        rows = jnp.concatenate([high, low, *asked, jnp.zeros((6, 128), F32)], axis=0)
        out[9] = rows[0:16].astype(out.dtype)
        out[10] = rows[16:32].astype(out.dtype)


def contract_kernel(meta, index, sign, *refs, scale, places):
    given, coeffs, wanted, plain, swapped, w_real, w_imag, total = (refs[:4], *refs[4:11])
    sums = jnp.zeros((9, 128), F32)
    for step, g in enumerate(given):
        tail = jnp.concatenate([g[9].astype(F32), g[10].astype(F32)], axis=0)
        sums = sums + (tail[0:9] + tail[9:18])
        for n, offset in enumerate(SOURCES):
            source = (meta[1] - NEAR * step - offset + 2 * places) % places
            wanted[source] = tail[18 + n : 19 + n]
    sums = sums * scale
    for a in range(3):
        tiles = [sum(g[3 * a + n].astype(F32) for g in given) * scale for n in range(3)]
        rows = [jnp.broadcast_to(sums[3 * a + n : 3 * a + n + 1], (16, 128)) for n in range(3)]
        turned = other_part(tiles)
        w_turned = other_part(rows)
        low = lanes_of((16, 128)) < 64
        real = [rows[0], jnp.where(low, rows[1], w_turned[1]), w_turned[2]]
        imag = [-w_turned[0], jnp.where(low, -w_turned[1], rows[1]), rows[2]]
        for alpha in range(4):
            i = 4 * a + alpha
            for n in range(3):
                for to, x in ((plain, tiles), (swapped, turned), (w_real, real), (w_imag, imag)):
                    to[i, n] = x[n] if alpha == 0 else pltpu.roll(x[n], 128 - alpha, 1)
    total[...] = jnp.zeros(total.shape, F32)

    def term(m, carry):
        first, second, out = (index[3 * m], index[3 * m + 1], index[3 * m + 2])
        signed = (2 * sign[m] - 1).astype(F32)
        value = plain[first] * w_real[second] + swapped[first] * w_imag[second]
        total[out] = total[out] + signed * value
        return carry

    lax.fori_loop(0, NTERM, term, 0, unroll=2)
    place = lanes_of((16, 128)) % 4
    for a in range(3):
        for n in range(3):
            moved = [total[4 * a, n]] + [
                pltpu.roll(total[4 * a + alpha, n], alpha, 1) for alpha in range(1, 4)
            ]
            coeffs[3 * a + n] = pick(place, moved).astype(BF16)


def join_kernel(meta, *refs):
    given, out = (refs[:8], refs[8])
    for offset, g in zip(SOURCES, given):
        slot = (meta[1] - offset + NEAR) % NEAR
        for n in range(9):
            out[n, slot] = g[n]


def rebuild_kernel(meta, ours, theirs, eig, table, wanted, *refs, scale):
    *outs, source, packed = refs
    step = pl.program_id(0)
    length = eig.shape[-1]

    @pl.when(step < 3)
    def _():
        dense = []
        for n in range(3):
            pair = [x[3 * step + n].astype(F32).reshape(-1, 128) for x in (ours, theirs)]
            dense.append(
                jnp.concatenate([pick(meta[2], pair), pick(meta[2], pair[::-1])], axis=0)
            )
        both = eig[:, 0].reshape(-1, length)
        turned = with_signs(other_part(dense))
        left = jnp.concatenate(
            [jnp.concatenate([x.T, y.T], axis=1) for x, y in zip(dense, turned)], axis=0
        ).astype(BF16)
        product = jnp.dot(left, both, preferred_element_type=F32)
        real = product[0:48]
        imag = product[192:240]
        for p in range(1, NMOM):
            cosine = table[p : p + 1, :]
            sine = table[NMOM + p : NMOM + p + 1, :]
            part_real = product[48 * p : 48 * p + 48]
            part_imag = product[192 + 48 * p : 240 + 48 * p]
            real = real + (cosine * part_real - sine * part_imag)
            imag = imag + (cosine * part_imag + sine * part_real)
        source[0, step] = (real * scale).astype(BF16)
        source[1, step] = (imag * scale).astype(BF16)

    @pl.when(step >= 3)
    def _():
        group = step - 3
        low_half = lanes_of((1, 128)) < 64
        segment = lanes_of((72, 128)) // 32
        sites = lax.broadcasted_iota(jnp.int32, (length, 128), 0)
        hots = []
        for t in range(2):
            row_a = wanted[4 * group + 2 * t]
            row_b = wanted[4 * group + 2 * t + 1]
            local_a = row_a * DIGIT + half_swap(row_a)
            local_b = half_swap(row_b) * DIGIT + row_b
            local = jnp.where(low_half, local_a, local_b).astype(jnp.int32)
            hots.append(jnp.where(sites == local, 1.0, 0.0).astype(BF16))
        hot = jnp.concatenate(hots, axis=1)
        picked = jnp.dot(source[...].reshape(-1, length), hot, preferred_element_type=F32)
        for t in range(2):
            blocks = [
                picked[72 * q : 72 * q + 72, 128 * t : 128 * t + 128] for q in range(4)
            ]
            for s in range(4):
                packed[4 * group + 2 * t + s // 2, s % 2] = pick(
                    segment,
                    [
                        blocks[q] if q == s else pltpu.roll(blocks[q], 32 * (q - s) % 128, 1)
                        for q in range(4)
                    ],
                ).astype(BF16)

    @pl.when(step == pl.num_programs(0) - 1)
    def _():
        places = packed.shape[0]

        def toward(offset):
            return packed[(meta[1] + offset + places) % places]

        outs[0][...] = toward(0)
        outs[1][...] = toward(2 * NEAR)
        outs[2][...] = toward(NEAR)
        outs[3][...] = toward(-NEAR)
        for hop, out in zip(HOPS, outs[4:]):
            out[0] = toward(hop)
            out[1] = toward(hop + NEAR if hop > 0 else hop - NEAR)


def collect_kernel(meta, own, across, *refs):
    ahead, behind, hops, keep, send = (refs[0:2], refs[2:4], refs[4:18], refs[18], refs[19])
    places = keep.shape[0]
    core = meta[2]

    def put(offset, chunk):
        source = (meta[1] - offset + 2 * places) % places
        keep[source] = chunk[core]
        send[source] = chunk[1 - core]

    put(0, own)
    put(2 * NEAR, across)
    for hop, given in zip(HOPS, hops):
        put(hop, given.at[0])
    for n in range(NEAR):
        reach = NEAR if n == 0 else 2 * NEAR - n
        put(reach, ahead[n // 4].at[n % 4])
        put(-reach, behind[n // 4].at[n % 4])


def place_kernel(meta, ours, theirs, out):
    segment = lanes_of((72, 128)) // 32
    for t in range(out.shape[-1] // 128):
        blocks = []
        for n in (2 * t, 2 * t + 1):
            pair = (ours[n].astype(F32), theirs[n].astype(F32))
            blocks += [pick(meta[2], pair), pick(meta[2], pair[::-1])]
        for q in range(4):
            mixed = pick(
                segment,
                [
                    blocks[s] if q == s else pltpu.roll(blocks[s], 32 * (s - q) % 128, 1)
                    for s in range(4)
                ],
            ).astype(BF16)
            for n in range(18):
                part, colour, j = ((18 * q + n) // 36, (18 * q + n) // 12 % 3, (18 * q + n) % 12)
                out[part, colour, j, :, 128 * t : 128 * t + 128] = mixed[4 * n : 4 * n + 4]


def shape_of(shape, dtype):
    return jax.ShapeDtypeStruct(shape, dtype)


def whole(count):
    return [pl.BlockSpec(memory_space=pltpu.VMEM)] * count


def small_call(kernel, scalars, arrays, outs, scratch=()):
    out_shape = [shape_of(*o) for o in outs]
    return pl.pallas_call(
        kernel,
        grid_spec=pltpu.PrefetchScalarGridSpec(
            num_scalar_prefetch=len(scalars),
            grid=(),
            in_specs=whole(len(arrays)),
            out_specs=whole(len(outs)),
            scratch_shapes=list(scratch),
        ),
        out_shape=out_shape,
    )(*scalars, *arrays)


def on_device(
    propagator, eigvecs, operator_weights, sink_time, term_index, term_sign, solver_order
):
    length = propagator.shape[-1]
    vectors = eigvecs.shape[2]
    places = lax.axis_size("z")
    devices = 2 * places
    z = lax.axis_index("z")
    core = lax.axis_index("core")
    meta = jnp.stack([sink_time[0], z, core]).astype(jnp.int32)
    scale_in = 1.0 / math.sqrt(3.0 * length * devices)
    scale_out = 1.0 / math.sqrt(NMOM * vectors)

    def shifted(x, offset):
        return lax.ppermute(x, "z", [(n, (n + offset) % places) for n in range(places)])

    def swapped(x):
        return lax.ppermute(x, "core", [(0, 1), (1, 0)])

    local = solver_order.reshape(4, NEAR, 2, 1, devices // 2) % length
    blank = jnp.zeros_like(local)
    digits = jnp.concatenate([local // DIGIT, blank, local % DIGIT, blank], axis=3).astype(F32)
    by_core = digits.transpose(2, 1, 0, 3, 4).reshape(2, NEAR, 4, 128)
    mine = lax.dynamic_index_in_dim(by_core, core, 0, keepdims=False)
    partners = lax.dynamic_index_in_dim(by_core, 1 - core, 0, keepdims=False)

    half = (vectors // 2 // 16, 16, 128)
    send, keep, weighted, table = pl.pallas_call(
        project_kernel,
        grid_spec=pltpu.PrefetchScalarGridSpec(
            num_scalar_prefetch=1,
            grid=(3,),
            in_specs=[
                pl.BlockSpec((2, 1, 12, 4, length), lambda a, m: (0, a, 0, 0, 0)),
                pl.BlockSpec((2, 1, vectors, length), lambda a, m: (0, a, 0, 0)),
                pl.BlockSpec((1, 2, vectors), lambda a, m: (m[0], 0, 0)),
                pl.BlockSpec(memory_space=pltpu.VMEM),
            ],
            out_specs=[
                pl.BlockSpec(memory_space=pltpu.VMEM),
                pl.BlockSpec((3, *half), lambda a, m: (a, 0, 0, 0)),
                pl.BlockSpec((1, 8, 128), lambda a, m: (a, 0, 0)),
                pl.BlockSpec((8, length), lambda a, m: (0, 0)),
            ],
            scratch_shapes=[
                pltpu.VMEM((384, length), BF16),
                pltpu.VMEM((2, *half), F32),
                pltpu.VMEM((2, 48, length), F32),
            ],
        ),
        out_shape=[
            shape_of((10, *half), F32),
            shape_of((9, *half), F32),
            shape_of((3, 8, 128), F32),
            shape_of((8, length), F32),
        ],
        name="project",
    )(meta, propagator.transpose(0, 1, 3, 2, 4), eigvecs, operator_weights, partners)

    message = (11, 16, 128)
    split = small_call(
        split_kernel,
        [meta],
        [keep, swapped(send), weighted, mine],
        [(message, F32)] + [(message, BF16)] * 7,
    )
    near = [split[0]] + [shifted(x, o) for x, o in zip(split[1:], NEAR_OFFSETS)]
    far = small_call(near_kernel, [meta], near, [(message, F32)] + [(message, BF16)] * 3)
    arrived = {0: far[0]} | {n: shifted(far[n], NEAR * n - places * (n == 3)) for n in (2, 1, 3)}
    wide = pltpu.VMEM((12, 3, 16, 128), F32)
    coeffs, places_wanted = small_call(
        functools.partial(contract_kernel, scale=scale_in, places=places),
        [meta, term_index.reshape(-1), term_sign],
        [arrived[n] for n in range(4)],
        [((9, 16, 128), BF16), ((places, 1, 128), F32)],
        [wide] * 5,
    )
    ours = [coeffs] + [shifted(coeffs, o) for o in NEAR_OFFSETS]
    (ours,) = small_call(join_kernel, [meta], ours, [((9, *half), BF16)])
    theirs = swapped(ours)

    chunk = (2, 72, 128)
    shapes = [chunk] * 4 + [(2, *chunk)] * 14
    own, across, ahead, behind, *hops = pl.pallas_call(
        functools.partial(rebuild_kernel, scale=scale_out),
        grid_spec=pltpu.PrefetchScalarGridSpec(
            num_scalar_prefetch=1,
            grid=(3 + devices // 8,),
            in_specs=whole(2)
            + [
                pl.BlockSpec(
                    (2, 1, vectors, length), lambda s, m: (0, jnp.minimum(s, 2), 0, 0)
                ),
                pl.BlockSpec(memory_space=pltpu.VMEM),
                pl.BlockSpec(memory_space=pltpu.VMEM),
            ],
            out_specs=whole(18),
            scratch_shapes=[
                pltpu.VMEM((2, 3, 48, length), BF16),
                pltpu.VMEM((places, *chunk), BF16),
            ],
        ),
        out_shape=[shape_of(x, BF16) for x in shapes],
        name="rebuild",
    )(meta, ours, theirs, eigvecs, table, places_wanted)
    passed = [shifted(x, hop) for x, hop in zip(hops, HOPS)]
    across = shifted(across, 2 * NEAR)
    ahead = [ahead] + [x[1] for x in passed[0::2]]
    behind = [behind] + [x[1] for x in passed[1::2]]
    ahead = [shifted(jnp.stack(ahead[4 * n : 4 * n + 4]), NEAR) for n in range(2)]
    behind = [shifted(jnp.stack(behind[4 * n : 4 * n + 4]), -NEAR) for n in range(2)]
    stacked = ((places, 72, 128), BF16)
    kept, sent = small_call(
        collect_kernel, [meta], [own, across, *ahead, *behind, *passed], [stacked] * 2
    )
    received = swapped(sent)
    tiles = 2
    moved = pl.BlockSpec((2 * tiles, 72, 128), lambda t, m: (t, 0, 0))
    placed = pl.pallas_call(
        place_kernel,
        grid_spec=pltpu.PrefetchScalarGridSpec(
            num_scalar_prefetch=1,
            grid=(length // (128 * tiles),),
            in_specs=[moved, moved],
            out_specs=pl.BlockSpec((2, 3, 12, 4, 128 * tiles), lambda t, m: (0, 0, 0, 0, t)),
        ),
        out_shape=shape_of((2, 3, 12, 4, length), BF16),
        name="place",
    )(meta, kept, received)
    return placed.transpose(0, 1, 3, 2, 4)


def solution(mesh):
    shape = (mesh.shape["grp"], mesh.shape["space"] // 2, 2)
    finer = Mesh(mesh.devices.reshape(shape), ("grp", "z", "core"))
    space = ("z", "core")
    in_specs = (
        P("grp", None, None, None, space),
        P("grp", None, None, space),
        P("grp", None, None),
        P("grp"),
        P(),
        P(),
        P(space),
    )
    out_specs = P("grp", None, None, None, space)
    return jax.shard_map(
        on_device, mesh=finer, in_specs=in_specs, out_specs=out_specs, check_vma=False
    )
```
